32 devices in a mesh: obs: 4 (over y, x), patch: 8 (over z, core).
Axes of the slice: x: 2, y: 2, z: 4, core: 2. Of those that a mesh axis runs over, the one named last changes fastest.
Arguments:
- green: float32 [5120, 5120], P('obs', 'patch'), may hold values from -0.078125 to 0.078125
- data: float32 [5120, 128], P('obs'), may hold values from -6 to 6
- neighbours: int32 [3, 5120], P(None, 'patch'), may hold values from 0 to 5119, as said below
- reg_weight: float32 [128], replicated, may hold values from 0.5 to 2
Outputs:
- slip: float32 [5120, 128], P('patch')
The draws below stay inside these ranges and needn't reach their ends.
Inputs may be any that keep to these rules, and one draw needn't show every extreme that they name: `neighbours`: entry (k, i) is a patch within 128 of i; an entry equal to i is padding. Distance 128 is reached in every draw.
All inputs are finite; a program needn't handle non-finite values.
Results may differ from the reference program's by a relative error of at most 0.0001.
Values sent between devices are 32-bit elements; how exact they have to be, the bound alone decides.
A program may use at most 64 MiB of HBM per device.

```python
import math
import jax
import jax.numpy as jnp
from jax import lax

EPOCHS = 128
BAND = 128
ITERS = 3
OBS = 5120
NPATCH = 5120


def draw_neighbours(key, part):
    key_offsets = jax.random.fold_in(key, 11)
    key_padding = jax.random.fold_in(key, 12)
    offsets = jax.random.randint(key_offsets, (3, NPATCH), -BAND, BAND + 1)
    padding = jax.random.randint(key_padding, (3, NPATCH), 0, 4) == 0
    offsets = jnp.where(padding, 0, offsets)
    indices = jnp.arange(NPATCH, dtype=jnp.int32)
    marked = indices % 37 == 5
    offsets = offsets.at[0].set(jnp.where(marked, -BAND, offsets[0]))
    offsets = offsets.at[1].set(jnp.where(marked, BAND, offsets[1]))
    return jnp.clip(indices[None, :] + offsets, 0, NPATCH - 1).astype(jnp.int32)


def level_of(key, extent, split, least, largest):
    level = 1.0
    for position, parts in split:
        draws = jax.random.uniform(jax.random.fold_in(jax.random.fold_in(key, 6), position), (parts,), jnp.float32, least / len(split), largest / len(split))
        level = level * jnp.repeat(jnp.exp(draws), extent[position] // parts).reshape((-1,) + (1,) * (len(extent) - 1 - position))
    return level


def gaussian(stream_key, dims, spread, most, shards=(), kind=jnp.bfloat16):
    loudness = level_of(stream_key, dims, shards, -0.22, 0.18) if shards else 1.0
    array = jax.random.normal(stream_key, dims, jnp.float32) * spread * loudness
    return jnp.minimum(jnp.maximum(array, -most), most).astype(kind)


def setup_inputs(seed: int = 0) -> dict:
    seeds = jax.random.split(jax.random.key(seed), 5)
    green = gaussian(seeds[0], (OBS, NPATCH), NPATCH ** -0.5, 0.078125, ((0, 4), (1, 8)), jnp.float32)
    data = gaussian(seeds[1], (OBS, EPOCHS), 1.0, 6.0, ((0, 4),), jnp.float32)
    neighbours = draw_neighbours(jax.random.fold_in(seeds[4], 71), 0)
    reg_weight = jnp.clip(jnp.exp(jax.random.uniform(seeds[3], (EPOCHS,), jnp.float32, math.log(0.5), math.log(2.0))), 0.5, 2.0)
    return {"green": green, "data": data, "neighbours": neighbours, "reg_weight": reg_weight}


def laplace(field, neighbours):
    return 4.0 * field - field[neighbours[0]] - field[neighbours[1]] - field[neighbours[2]]


def laplace_t(values, neighbours):
    result = 4.0 * values
    for slot in range(3):
        result = result.at[neighbours[slot]].add(-values)
    return result


def transposed(green, residual):
    return lax.dot_general(green, residual, (((0,), (0,)), ((), ())), precision=lax.Precision.HIGHEST, preferred_element_type=jnp.float32)


def reference(green, data, neighbours, reg_weight):
    slip = jnp.zeros((NPATCH, EPOCHS), jnp.float32)
    residual = data
    reg_resid = jnp.zeros((NPATCH, EPOCHS), jnp.float32)
    gradient = transposed(green, data)
    grad_norm = jnp.sum(gradient * gradient, axis=0)
    direction = gradient
    for iteration in range(ITERS):
        image = jnp.dot(green, direction, precision=lax.Precision.HIGHEST, preferred_element_type=jnp.float32)
        reg_image = reg_weight * laplace(direction, neighbours)
        curvature = jnp.sum(image * image, axis=0) + jnp.sum(reg_image * reg_image, axis=0)
        step_size = grad_norm / curvature
        slip = slip + step_size * direction
        if iteration + 1 < ITERS:
            residual = residual - step_size * image
            reg_resid = reg_resid - step_size * reg_image
            gradient = transposed(green, residual) + reg_weight * laplace_t(reg_resid, neighbours)
            next_norm = jnp.sum(gradient * gradient, axis=0)
            direction = gradient + (next_norm / grad_norm) * direction
            grad_norm = next_norm
    return slip
```

```python
import functools
import math

import jax
import jax.numpy as jnp
from jax import lax
from jax.experimental import pallas as pl
from jax.experimental.pallas import tpu as pltpu
from jax.sharding import PartitionSpec as P

BAND = 128
ITERS = 3
MESH = pl.DeviceIdType.MESH
F32 = jnp.float32
BF16 = jnp.bfloat16


def dot(a, b):
    return lax.dot_general(a, b, (((1,), (0,)), ((), ())), preferred_element_type=F32)


def split(x):
    hi = x.astype(BF16)
    return hi, (x - hi.astype(F32)).astype(BF16)


def kernel(n_obs, n_patch, nc, bc, green, data, nb, rw, out,
           ghi, glo, gthi, gtlo, lm, lmt, cat_d, cat_r, cat_e,
           d, g, a, wext, slip, sq,
           pf, s, rd, sr, sl, rl, rr, img, bb, br, hal, wr, scs, scr, pls, plr,
           sem_d, sem_l, sem_r, sem_i, sem_b, sem_h, sem_w, sem_s, sem_p, sem_n):
    rows, cols = green.shape
    E = data.shape[1]
    R = rows // 2 // nc
    BR = cols // bc
    CB = cols // BAND
    nz = n_patch // 2
    nbit = n_obs.bit_length() - 1
    obs = lax.axis_index("obs")
    pat = lax.axis_index("patch")
    z = pat // 2
    c = pat % 2
    other = 1 - c
    partner = z * 2 + other
    has_l, has_r = pat > 0, pat < n_patch - 1
    up, down = z < nz - 1, z > 0
    weight = rw[...]

    def at(o, q):
        return (o, q)

    def rcopy(src, dst, sems, dev):
        return pltpu.make_async_remote_copy(
            src_ref=src, dst_ref=dst, send_sem=sems[0], recv_sem=sems[1],
            device_id=dev, device_id_type=MESH)

    def pair(sem, *idx):
        return sem.at[(0,) + idx], sem.at[(1,) + idx]

    barrier = pltpu.get_barrier_semaphore()

    @pl.loop(1, n_patch)
    def _(i):
        pl.semaphore_signal(barrier, inc=1, device_id=at(obs, (pat + i) % n_patch), device_id_type=MESH)

    n_plane = 2 * n_obs

    def plane(i):
        q = (obs * 2 + c + i) % n_plane
        return q // 2, z * 2 + q % 2

    @pl.loop(1, n_plane)
    def _(i):
        pl.semaphore_signal(barrier, inc=1, device_id=plane(i), device_id_type=MESH)

    nblk = rows // BAND

    @pl.loop(0, nblk)
    def _(i):
        r0 = pl.multiple_of(i * BAND, BAND)
        block = green[pl.ds(r0, BAND), :]
        hi, lo = split(block)
        ghi[pl.ds(r0, BAND), :] = hi
        glo[pl.ds(r0, BAND), :] = lo
        hi, lo = split(block.T)
        for j in range(bc):
            gthi[j, :, pl.ds(r0, BAND)] = hi[j * BR:(j + 1) * BR]
            gtlo[j, :, pl.ds(r0, BAND)] = lo[j * BR:(j + 1) * BR]
        hi, lo = split(data[pl.ds(r0, BAND), :])
        cat_r[pl.ds(r0, BAND), 0:E] = hi
        cat_r[pl.ds(r0, BAND), E:2 * E] = lo

    scs[...] = jnp.zeros((ITERS, 8, E), F32)
    zero_c = jnp.zeros((nc, R, E), F32)
    zero_h = jnp.zeros((BAND, E), F32)

    @pl.when(z == 0)
    def _():
        for it in range(ITERS):
            rl[it] = zero_c

    @pl.when(z == nz - 1)
    def _():
        for it in range(ITERS):
            rr[it] = zero_c

    @pl.when(pat == 0)
    def _():
        for it in range(ITERS):
            hal[it, 0] = zero_h
        for it in range(ITERS - 1):
            wr[it, 0] = zero_h

    @pl.when(pat == n_patch - 1)
    def _():
        for it in range(ITERS):
            hal[it, 1] = zero_h
        for it in range(ITERS - 1):
            wr[it, 1] = zero_h

    def build_laplace():
        @pl.loop(0, CB + 2)
        def _(j):
            r0 = pl.multiple_of(j * BAND, BAND)
            col = lax.broadcasted_iota(jnp.int32, (BAND, cols), 0) + j * BAND
            own = lax.broadcasted_iota(jnp.int32, (BAND, cols), 1) + BAND
            m = jnp.where(col == own, 4.0, 0.0)
            col = col + (pat * cols - BAND)
            for k in range(3):
                m = m - jnp.where(col == nb[k:k + 1, :], 1.0, 0.0)
            lmt[pl.ds(r0, BAND), :] = m.astype(BF16)
            lm[:, pl.ds(r0, BAND)] = m.T.astype(BF16)

    pl.semaphore_wait(barrier, n_patch - 1 + n_plane - 1)

    def bit_partner(p, j):
        b0, b1 = 1 << p, 1 << (nbit - 1 - p)
        bit = b0 + (j % 2) * (b1 - b0)
        return at(obs + bit * (1 - 2 * ((obs // bit) % 2)), pat)

    def bcopy(b, p, j):
        return rcopy(bb.at[b, p, j], br.at[b, p, j], pair(sem_b, b, p, j), bit_partner(p, j))

    def backward(b, hook, dst):
        @pl.loop(0, bc)
        def _(j):
            y = dot(gthi[j], cat_r[...])
            bb[b, 0, j] = y[:, :E] + y[:, E:] + dot(gtlo[j], cat_r[:, 0:E])
            bcopy(b, 0, j).start()

        hook()
        for p in range(1, nbit):
            @pl.loop(0, bc)
            def _(j):
                bcopy(b, p - 1, j).wait_recv()
                bb[b, p, j] = bb[b, p - 1, j] + br[b, p - 1, j]
                bcopy(b, p, j).start()

        @pl.loop(0, bc)
        def _(j):
            bcopy(b, nbit - 1, j).wait_recv()
            dst[pl.ds(pl.multiple_of(j * BR, BR), BR), :] = bb[b, nbit - 1, j] + br[b, nbit - 1, j]

        for p in range(nbit):
            @pl.loop(0, bc)
            def _(j):
                bcopy(b, p, j).wait_send()

    def dcopy(it, k):
        return rcopy(pf.at[k], rd.at[it, k], pair(sem_d, it, k), at(obs, partner))

    def rcopy_up(it, src, k):
        return rcopy(src.at[k], rl.at[it, k], pair(sem_l, it, k), at(obs, pat + 2))

    def rcopy_down(it, src, k):
        return rcopy(src.at[k], rr.at[it, k], pair(sem_r, it, k), at(obs, pat - 2))

    def icopy(it, k):
        return rcopy(img.at[it, c, k], img.at[it, c, k], pair(sem_i, it, k), at(obs, partner))

    def put_cat(h, k, value):
        hi, lo = split(value)
        r0 = pl.multiple_of((h * nc + k) * R, R)
        cat_r[pl.ds(r0, R), 0:E] = hi
        cat_r[pl.ds(r0, R), E:2 * E] = lo

    def hcopy_r(it):
        return rcopy(d.at[pl.ds(cols - BAND, BAND)], hal.at[it, 0], pair(sem_h, it, 0), at(obs, pat + 1))

    def hcopy_l(it):
        return rcopy(d.at[pl.ds(0, BAND)], hal.at[it, 1], pair(sem_h, it, 1), at(obs, pat - 1))

    def forward(it, hook):
        last = it == ITERS - 1

        @pl.when(has_r)
        def _():
            hcopy_r(it).start()

        @pl.when(has_l)
        def _():
            hcopy_l(it).start()

        hi, lo = split(d[...])
        cat_d[:, 0:E] = hi
        cat_d[:, E:2 * E] = lo

        def part(h, k):
            r0 = pl.multiple_of((h * nc + k) * R, R)
            y = dot(ghi[pl.ds(r0, R), :], cat_d[...])
            return y[:, :E] + y[:, E:] + dot(glo[pl.ds(r0, R), :], cat_d[:, 0:E])

        @pl.loop(0, nc)
        def _(k):
            pf[k] = part(other, k)
            dcopy(it, k).start()

        @pl.loop(0, nc)
        def _(k):
            y = part(c, k)
            dcopy(it, k).wait_recv()
            s[k] = y + rd[it, k]

            @pl.when(z == 0)
            def _():
                rcopy_up(it, s, k).start()

            @pl.when(z == nz - 1)
            def _():
                rcopy_down(it, s, k).start()

        def chain(t):
            kl = t - z
            kr = t - (nz - 1 - z)
            kt = t - jnp.maximum(z, nz - 1 - z)

            @pl.when(down & (kl >= 0) & (kl < nc))
            def _():
                rcopy_up(it, sr, kl).wait_recv()

                @pl.when(up)
                def _():
                    sr[kl] = rl[it, kl] + s[kl]
                    rcopy_up(it, sr, kl).start()

            @pl.when(up & (kr >= 0) & (kr < nc))
            def _():
                rcopy_down(it, sl, kr).wait_recv()

                @pl.when(down)
                def _():
                    sl[kr] = rr[it, kr] + s[kr]
                    rcopy_down(it, sl, kr).start()

            @pl.when((kt >= 0) & (kt < nc))
            def _():
                total = rl[it, kt] + s[kt] + rr[it, kt]
                if last:
                    sq[...] += jnp.sum((total * total).reshape(R // 8, 8, E), axis=0)
                else:
                    img[it, c, kt] = total
                    icopy(it, kt).start()
                    put_cat(c, kt, total)

        if last:
            sq[...] = jnp.zeros((8, E), F32)
            hook()
        pl.loop(1, nc + nz - 1)(chain)

        if not last:
            @pl.loop(0, nc)
            def _(k):
                icopy(it, k).wait_recv()
                put_cat(other, k, img[it, other, k])

        @pl.loop(0, nc)
        def _(k):
            dcopy(it, k).wait_send()
            if not last:
                icopy(it, k).wait_send()

            @pl.when(up)
            def _():
                rcopy_up(it, sr, k).wait_send()

            @pl.when(down)
            def _():
                rcopy_down(it, sl, k).wait_send()

    def laplace(it):
        @pl.when(has_l)
        def _():
            hcopy_r(it).wait_recv()

        @pl.when(has_r)
        def _():
            hcopy_l(it).wait_recv()

        for r0, n, v in ((0, BAND, hal[it, 0]), (BAND, cols, d[...]), (BAND + cols, BAND, hal[it, 1])):
            hi, lo = split(v)
            cat_e[r0:r0 + n, 0:E] = hi
            cat_e[r0:r0 + n, E:2 * E] = lo

        @pl.when(has_r)
        def _():
            hcopy_r(it).wait_send()

        @pl.when(has_l)
        def _():
            hcopy_l(it).wait_send()

    def lap_rows(i):
        r0 = pl.multiple_of(i * BAND, BAND)
        y = dot(lm[pl.ds(r0, BAND), :], cat_e[...])
        return r0, weight * (y[:, :E] + y[:, E:])

    def wcopy_l(it):
        return rcopy(wext.at[pl.ds(0, BAND)], wr.at[it, 1], pair(sem_w, it, 1), at(obs, pat - 1))

    def wcopy_r(it):
        return rcopy(wext.at[pl.ds(BAND + cols, BAND)], wr.at[it, 0], pair(sem_w, it, 0), at(obs, pat + 1))

    def reg_start(it):
        laplace(it)

        @pl.loop(0, CB)
        def _(i):
            r0, u = lap_rows(i)
            hi, lo = split(u)
            cat_d[pl.ds(r0, BAND), 0:E] = hi
            cat_d[pl.ds(r0, BAND), E:2 * E] = lo

        @pl.loop(0, CB + 2)
        def _(i):
            r0 = pl.multiple_of(i * BAND, BAND)
            y = dot(lmt[pl.ds(r0, BAND), :], cat_d[...])
            wext[pl.ds(r0, BAND), :] = weight * (y[:, :E] + y[:, E:])

        @pl.when(has_l)
        def _():
            wcopy_l(it).start()

        @pl.when(has_r)
        def _():
            wcopy_r(it).start()

    def reg_end(it):
        a[...] += wext[BAND:BAND + cols, :]

        @pl.when(has_l)
        def _():
            wcopy_r(it).wait_recv()

        @pl.when(has_r)
        def _():
            wcopy_l(it).wait_recv()

        a[0:BAND, :] += wr[it, 0]
        a[cols - BAND:cols, :] += wr[it, 1]

        @pl.when(has_l)
        def _():
            wcopy_l(it).wait_send()

        @pl.when(has_r)
        def _():
            wcopy_r(it).wait_send()

    def scopy(it, slot, q):
        return rcopy(scs.at[it], scr.at[it, slot], (sem_s.at[0, it, q], sem_s.at[1, it, slot]), at(obs, q))

    def sums_start(it):
        scr[it, pat] = scs[it]

        @pl.loop(1, n_patch)
        def _(i):
            scopy(it, pat, (pat + i) % n_patch).start()

    def sums_end(it):
        @pl.loop(1, n_patch)
        def _(i):
            q = (pat + i) % n_patch
            scopy(it, q, q).wait_recv()

        @pl.loop(1, n_patch)
        def _(i):
            q = (pat + i) % n_patch
            scopy(it, pat, q).wait_send()

        return jnp.sum(scr[it], axis=0)

    def pcopy(slot, i):
        o, q = plane(i)
        return rcopy(pls, plr.at[slot], (sem_p.at[i], sem_n.at[slot]), (o, q))

    def rowsum(x):
        return jnp.sum(x, axis=0, keepdims=True)

    backward(0, build_laplace, g)
    d[...] = g[...]
    norm = None
    for it in range(ITERS - 1):
        forward(it, None)
        backward(it + 1, functools.partial(reg_start, it), a)
        reg_end(it)
        gv, dv, av = g[...], d[...], a[...]
        scs[it, 0:1, :] = rowsum(gv * gv)
        scs[it, 1:2, :] = rowsum(dv * av)
        scs[it, 2:3, :] = rowsum(gv * av)
        scs[it, 3:4, :] = rowsum(av * av)
        sums_start(it)
        tot = sums_end(it)
        if norm is None:
            norm = tot[0:1]
        step = norm / tot[1:2]
        after = norm - 2.0 * step * tot[2:3] + step * step * tot[3:4]
        if it == 0:
            slip[...] = step * d[...]
        else:
            slip[...] += step * d[...]
        g[...] = g[...] - step * a[...]
        d[...] = g[...] + (after / norm) * d[...]
        norm = after

    last = ITERS - 1

    def reg_norm():
        laplace(last)
        scs[last] = jnp.zeros((8, E), F32)

        @pl.loop(0, CB)
        def _(i):
            _, u = lap_rows(i)
            scs[last] += jnp.sum((u * u).reshape(BAND // 8, 8, E), axis=0)

        sums_start(last)

    forward(last, reg_norm)
    me = obs * 2 + c
    pls[...] = sq[...]
    plr[me] = sq[...]

    @pl.loop(1, n_plane)
    def _(i):
        pcopy(me, i).start()

    reg = rowsum(sums_end(last))

    @pl.loop(1, n_plane)
    def _(i):
        pcopy((me + i) % n_plane, i).wait_recv()

    curvature = rowsum(jnp.sum(plr[...], axis=0)) + reg
    out[...] = slip[...] + (norm / curvature) * d[...]

    @pl.loop(1, n_plane)
    def _(i):
        pcopy(me, i).wait_send()


def shards(green, data, neighbours, reg_weight):
    rows, cols = green.shape
    E = data.shape[1]
    n_obs, n_patch = lax.axis_size("obs"), lax.axis_size("patch")
    nbit = n_obs.bit_length() - 1
    nc = rows // 2 // 128
    bc = 4
    R, BR, ext = rows // 2 // nc, cols // bc, cols + 2 * BAND
    V = pltpu.VMEM
    D = pltpu.SemaphoreType.DMA
    scratch = [
        V((rows, cols), BF16), V((rows, cols), BF16),
        V((bc, BR, rows), BF16), V((bc, BR, rows), BF16),
        V((cols, ext), BF16), V((ext, cols), BF16),
        V((cols, 2 * E), BF16), V((rows, 2 * E), BF16), V((ext, 2 * E), BF16),
        V((cols, E), F32), V((cols, E), F32), V((cols, E), F32), V((ext, E), F32), V((cols, E), F32),
        V((8, E), F32),
        V((nc, R, E), F32), V((nc, R, E), F32), V((ITERS, nc, R, E), F32),
        V((nc, R, E), F32), V((nc, R, E), F32),
        V((ITERS, nc, R, E), F32), V((ITERS, nc, R, E), F32),
        V((ITERS - 1, 2, nc, R, E), F32),
        V((ITERS, nbit, bc, BR, E), F32), V((ITERS, nbit, bc, BR, E), F32),
        V((ITERS, 2, BAND, E), F32), V((ITERS - 1, 2, BAND, E), F32),
        V((ITERS, 8, E), F32), V((ITERS, n_patch, 8, E), F32),
        V((8, E), F32), V((2 * n_obs, 8, E), F32),
        D((2, ITERS, nc)), D((2, ITERS, nc)), D((2, ITERS, nc)), D((2, ITERS - 1, nc)),
        D((2, ITERS, nbit, bc)), D((2, ITERS, 2)), D((2, ITERS - 1, 2)),
        D((2, ITERS, n_patch)), D((2 * n_obs,)), D((2 * n_obs,)),
    ]
    return pl.pallas_call(
        functools.partial(kernel, n_obs, n_patch, nc, bc),
        out_shape=jax.ShapeDtypeStruct((cols, E), F32),
        in_specs=[pl.BlockSpec(memory_space=pltpu.VMEM)] * 4,
        out_specs=pl.BlockSpec(memory_space=pltpu.VMEM),
        scratch_shapes=scratch,
        compiler_params=pltpu.CompilerParams(
            collective_id=0, has_side_effects=True, vmem_limit_bytes=56 * 1024 * 1024),
    )(green, data, neighbours, reg_weight.reshape(1, E))


def solution(mesh):
    in_specs = (P("obs", "patch"), P("obs", None), P(None, "patch"), P())
    return jax.shard_map(shards, mesh=mesh, in_specs=in_specs, out_specs=P("patch", None), check_vma=False)
```

```python
import functools
import math

import jax
import jax.numpy as jnp
from jax import lax
from jax.experimental import pallas as pl
from jax.experimental.pallas import tpu as pltpu
from jax.sharding import PartitionSpec as P

BAND = 128
ITERS = 3
MESH = pl.DeviceIdType.MESH
F32 = jnp.float32
BF16 = jnp.bfloat16


def dot(a, b):
    return lax.dot_general(a, b, (((1,), (0,)), ((), ())), preferred_element_type=F32)


def split(x):
    hi = x.astype(BF16)
    return hi, (x - hi.astype(F32)).astype(BF16)


def kernel(n_obs, n_patch, nc, bc, green, data, nb, rw, out,
           ghi, glo, gthi, gtlo, lm, lmt, cat_d, cat_r, cat_e,
           d, g, a, wext, slip, sq, hd, hg, qd, qg,
           pf, s, rd, sr, sl, rl, rr, img, bb, br, hal, wr, scs, scr, pls, plr,
           sem_d, sem_l, sem_r, sem_i, sem_b, sem_h, sem_w, sem_s, sem_p, sem_n):
    rows, cols = green.shape
    E = data.shape[1]
    R = rows // 2 // nc
    BR = cols // bc
    half = rows // 2
    per = 4
    lag = 4
    CB = cols // BAND
    nz = n_patch // 2
    nbit = n_obs.bit_length() - 1
    obs = lax.axis_index("obs")
    pat = lax.axis_index("patch")
    z = pat // 2
    c = pat % 2
    other = 1 - c
    partner = z * 2 + other
    has_l, has_r = pat > 0, pat < n_patch - 1
    up, down = z < nz - 1, z > 0
    weight = rw[...]

    def at(o, q):
        return (o, q)

    def rcopy(src, dst, sems, dev):
        return pltpu.make_async_remote_copy(
            src_ref=src, dst_ref=dst, send_sem=sems[0], recv_sem=sems[1],
            device_id=dev, device_id_type=MESH)

    def pair(sem, *idx):
        return sem.at[(0,) + idx], sem.at[(1,) + idx]

    barrier = pltpu.get_barrier_semaphore()

    @pl.loop(1, n_patch)
    def _(i):
        pl.semaphore_signal(barrier, inc=1, device_id=at(obs, (pat + i) % n_patch), device_id_type=MESH)

    n_plane = 2 * n_obs

    def plane(i):
        q = (obs * 2 + c + i) % n_plane
        return q // 2, z * 2 + q % 2

    @pl.loop(1, n_plane)
    def _(i):
        pl.semaphore_signal(barrier, inc=1, device_id=plane(i), device_id_type=MESH)

    nblk = rows // BAND

    @pl.loop(0, nblk)
    def _(i):
        r0 = pl.multiple_of(i * BAND, BAND)
        block = green[pl.ds(r0, BAND), :]
        hi, lo = split(block)
        ghi[pl.ds(r0, BAND), :] = hi
        glo[pl.ds(r0, BAND), :] = lo
        hi, lo = split(block.T)
        gthi[:, pl.ds(r0, BAND)] = hi
        gtlo[:, pl.ds(r0, BAND)] = lo
        hi, lo = split(data[pl.ds(r0, BAND), :])
        cat_r[pl.ds(r0, BAND), 0:E] = hi
        cat_r[pl.ds(r0, BAND), E:2 * E] = lo

    scs[...] = jnp.zeros((ITERS, 8, E), F32)
    zero_c = jnp.zeros((nc, R, E), F32)
    zero_h = jnp.zeros((BAND, E), F32)

    @pl.when(z == 0)
    def _():
        for it in range(ITERS):
            rl[it] = zero_c

    @pl.when(z == nz - 1)
    def _():
        for it in range(ITERS):
            rr[it] = zero_c

    @pl.when(pat == 0)
    def _():
        for it in range(ITERS):
            hal[it, 0] = zero_h
        for it in range(ITERS - 1):
            wr[it, 0] = zero_h

    @pl.when(pat == n_patch - 1)
    def _():
        for it in range(ITERS):
            hal[it, 1] = zero_h
        for it in range(ITERS - 1):
            wr[it, 1] = zero_h

    def build_laplace():
        @pl.loop(0, CB + 2)
        def _(j):
            r0 = pl.multiple_of(j * BAND, BAND)
            col = lax.broadcasted_iota(jnp.int32, (BAND, cols), 0) + j * BAND
            own = lax.broadcasted_iota(jnp.int32, (BAND, cols), 1) + BAND
            m = jnp.where(col == own, 4.0, 0.0)
            col = col + (pat * cols - BAND)
            for k in range(3):
                m = m - jnp.where(col == nb[k:k + 1, :], 1.0, 0.0)
            lmt[pl.ds(r0, BAND), :] = m.astype(BF16)
            lm[:, pl.ds(r0, BAND)] = m.T.astype(BF16)

    pl.semaphore_wait(barrier, n_patch - 1 + n_plane - 1)

    def bit_partner(p, j):
        b0, b1 = 1 << p, 1 << (nbit - 1 - p)
        bit = b0 + (j % 2) * (b1 - b0)
        return at(obs + bit * (1 - 2 * ((obs // bit) % 2)), pat)

    def bcopy(b, p, j):
        return rcopy(bb.at[b, p, j], br.at[b, p, j], pair(sem_b, b, p, j), bit_partner(p, j))

    def backward(b, hook, dst):
        for m in range(0, bc, per):
            y = dot(gthi[m * BR:(m + per) * BR, :], cat_r[...])
            y = y[:, :E] + y[:, E:] + dot(gtlo[m * BR:(m + per) * BR, :], cat_r[:, 0:E])
            bb[b, 0, m:m + per] = y.reshape(per, BR, E)
            for j in range(m, m + per):
                bcopy(b, 0, j).start()

        hook()
        for p in range(1, nbit):
            @pl.loop(0, bc)
            def _(j):
                bcopy(b, p - 1, j).wait_recv()
                bb[b, p, j] = bb[b, p - 1, j] + br[b, p - 1, j]
                bcopy(b, p, j).start()

        @pl.loop(0, bc)
        def _(j):
            bcopy(b, nbit - 1, j).wait_recv()
            dst[pl.ds(pl.multiple_of(j * BR, BR), BR), :] = bb[b, nbit - 1, j] + br[b, nbit - 1, j]

        for p in range(nbit):
            @pl.loop(0, bc)
            def _(j):
                bcopy(b, p, j).wait_send()

    def dcopy(it, k):
        return rcopy(pf.at[k], rd.at[it, k], pair(sem_d, it, k), at(obs, partner))

    def rcopy_up(it, src, k):
        return rcopy(src.at[k], rl.at[it, k], pair(sem_l, it, k), at(obs, pat + 2))

    def rcopy_down(it, src, k):
        return rcopy(src.at[k], rr.at[it, k], pair(sem_r, it, k), at(obs, pat - 2))

    def icopy(it, k):
        return rcopy(img.at[it, c, k], img.at[it, c, k], pair(sem_i, it, k), at(obs, partner))

    def put_cat(h, k, value):
        hi, lo = split(value)
        r0 = pl.multiple_of((h * nc + k) * R, R)
        cat_r[pl.ds(r0, R), 0:E] = hi
        cat_r[pl.ds(r0, R), E:2 * E] = lo

    def hcopy_r(it):
        return rcopy((a if it else g).at[pl.ds(cols - BAND, BAND)], hal.at[it, 0], pair(sem_h, it, 0), at(obs, pat + 1))

    def hcopy_l(it):
        return rcopy((a if it else g).at[pl.ds(0, BAND)], hal.at[it, 1], pair(sem_h, it, 1), at(obs, pat - 1))

    def forward(it, sums, hook):
        last = it == ITERS - 1

        @pl.when(has_r)
        def _():
            hcopy_r(it).start()

        @pl.when(has_l)
        def _():
            hcopy_l(it).start()

        hi, lo = split((a if it else g)[...])
        cat_d[:, 0:E] = hi
        cat_d[:, E:2 * E] = lo
        sums()

        def part(h):
            r0 = pl.multiple_of(h * half, half)
            y = dot(ghi[pl.ds(r0, half), :], cat_d[...])
            y = y[:, :E] + y[:, E:] + dot(glo[pl.ds(r0, half), :], cat_d[:, 0:E])
            return y.reshape(nc, R, E)

        pf[...] = part(other)

        @pl.loop(0, nc)
        def _(k):
            dcopy(it, k).start()

        s[...] = part(c)

        @pl.loop(0, nc)
        def _(k):
            dcopy(it, k).wait_recv()
            s[k] += rd[it, k]

            @pl.when(z == 0)
            def _():
                rcopy_up(it, s, k).start()

            @pl.when(z == nz - 1)
            def _():
                rcopy_down(it, s, k).start()

        def chain(t, ends=True):
            kl = t - lag * z
            kr = t - lag * (nz - 1 - z)
            kt = t - lag * jnp.maximum(z, nz - 1 - z)

            @pl.when(down & (kl >= 0) & (kl < nc))
            def _():
                rcopy_up(it, sr, kl).wait_recv()

                @pl.when(up)
                def _():
                    sr[kl] = rl[it, kl] + s[kl]
                    rcopy_up(it, sr, kl).start()

            @pl.when(up & (kr >= 0) & (kr < nc))
            def _():
                rcopy_down(it, sl, kr).wait_recv()

                @pl.when(down)
                def _():
                    sl[kr] = rr[it, kr] + s[kr]
                    rcopy_down(it, sl, kr).start()

            if not ends:
                return

            @pl.when((kt >= 0) & (kt < nc))
            def _():
                total = rl[it, kt] + s[kt] + rr[it, kt]
                if it:
                    step, ratio = scalars
                    rest = qg[kt] - step * total
                    total = rest + ratio * qd[kt]
                if not last:
                    qg[kt] = rest if it else total
                    qd[kt] = total
                if last:
                    sq[...] += jnp.sum((total * total).reshape(R // 8, 8, E), axis=0)
                else:
                    img[it, c, kt] = total
                    icopy(it, kt).start()
                    put_cat(c, kt, total)

        if last:
            sq[...] = jnp.zeros((8, E), F32)
        pl.loop(lag, lag * (nz // 2))(functools.partial(chain, ends=False))
        scalars = hook()
        pl.loop(lag * (nz // 2), nc + lag * (nz - 1))(chain)

        if not last:
            @pl.loop(0, nc)
            def _(k):
                icopy(it, k).wait_recv()
                put_cat(other, k, img[it, other, k])

        @pl.loop(0, nc)
        def _(k):
            dcopy(it, k).wait_send()
            if not last:
                icopy(it, k).wait_send()

            @pl.when(up)
            def _():
                rcopy_up(it, sr, k).wait_send()

            @pl.when(down)
            def _():
                rcopy_down(it, sl, k).wait_send()

    def halo_wait(it):
        @pl.when(has_l)
        def _():
            hcopy_r(it).wait_recv()

        @pl.when(has_r)
        def _():
            hcopy_l(it).wait_recv()

        @pl.when(has_r)
        def _():
            hcopy_r(it).wait_send()

        @pl.when(has_l)
        def _():
            hcopy_l(it).wait_send()

    def laplace():
        for r0, n, v in ((0, BAND, hd[0]), (BAND, cols, d[...]), (BAND + cols, BAND, hd[1])):
            hi, lo = split(v)
            cat_e[r0:r0 + n, 0:E] = hi
            cat_e[r0:r0 + n, E:2 * E] = lo

    def lap_rows(i):
        r0 = pl.multiple_of(i * BAND, BAND)
        y = dot(lm[pl.ds(r0, BAND), :], cat_e[...])
        return r0, weight * (y[:, :E] + y[:, E:])

    def wcopy_l(it):
        return rcopy(wext.at[pl.ds(0, BAND)], wr.at[it, 1], pair(sem_w, it, 1), at(obs, pat - 1))

    def wcopy_r(it):
        return rcopy(wext.at[pl.ds(BAND + cols, BAND)], wr.at[it, 0], pair(sem_w, it, 0), at(obs, pat + 1))

    def reg_start(it):
        laplace()

        @pl.loop(0, CB)
        def _(i):
            r0, u = lap_rows(i)
            hi, lo = split(u)
            cat_d[pl.ds(r0, BAND), 0:E] = hi
            cat_d[pl.ds(r0, BAND), E:2 * E] = lo

        @pl.loop(0, CB + 2)
        def _(i):
            r0 = pl.multiple_of(i * BAND, BAND)
            y = dot(lmt[pl.ds(r0, BAND), :], cat_d[...])
            wext[pl.ds(r0, BAND), :] = weight * (y[:, :E] + y[:, E:])

        @pl.when(has_l)
        def _():
            wcopy_l(it).start()

        @pl.when(has_r)
        def _():
            wcopy_r(it).start()

    def reg_end(it):
        a[...] += wext[BAND:BAND + cols, :]

        @pl.when(has_l)
        def _():
            wcopy_r(it).wait_recv()

        @pl.when(has_r)
        def _():
            wcopy_l(it).wait_recv()

        a[0:BAND, :] += wr[it, 0]
        a[cols - BAND:cols, :] += wr[it, 1]

        @pl.when(has_l)
        def _():
            wcopy_l(it).wait_send()

        @pl.when(has_r)
        def _():
            wcopy_r(it).wait_send()

    def scopy(it, slot, q):
        return rcopy(scs.at[it], scr.at[it, slot], (sem_s.at[0, it, q], sem_s.at[1, it, slot]), at(obs, q))

    def sums_start(it):
        scr[it, pat] = scs[it]

        @pl.loop(1, n_patch)
        def _(i):
            scopy(it, pat, (pat + i) % n_patch).start()

    def sums_end(it):
        @pl.loop(1, n_patch)
        def _(i):
            q = (pat + i) % n_patch
            scopy(it, q, q).wait_recv()

        @pl.loop(1, n_patch)
        def _(i):
            q = (pat + i) % n_patch
            scopy(it, pat, q).wait_send()

        return jnp.sum(scr[it], axis=0)

    def pcopy(slot, i):
        o, q = plane(i)
        return rcopy(pls, plr.at[slot], (sem_p.at[i], sem_n.at[slot]), (o, q))

    def rowsum(x):
        return jnp.sum(x, axis=0, keepdims=True)

    norms = []

    def dots(it):
        gv, dv, av = g[...], d[...], a[...]
        scs[it, 0:1, :] = rowsum(gv * gv)
        scs[it, 1:2, :] = rowsum(dv * av)
        scs[it, 2:3, :] = rowsum(gv * av)
        scs[it, 3:4, :] = rowsum(av * av)
        sums_start(it)

    def first():
        halo_wait(0)
        hg[...] = hal[0]
        hd[...] = hal[0]

    def advance(it):
        tot = sums_end(it - 1)
        if it == 1:
            norms.append(tot[0:1])
        norm = norms[-1]
        step = norm / tot[1:2]
        after = norm - 2.0 * step * tot[2:3] + step * step * tot[3:4]
        ratio = after / norm
        norms.append(after)
        halo_wait(it)
        if it == 1:
            slip[...] = step * d[...]
        else:
            slip[...] += step * d[...]
        g[...] = g[...] - step * a[...]
        d[...] = g[...] + ratio * d[...]
        hg[...] = hg[...] - step * hal[it]
        hd[...] = hg[...] + ratio * hd[...]
        if it == ITERS - 1:
            laplace()

            @pl.loop(0, CB)
            def _(i):
                _, u = lap_rows(i)
                scs[it] += jnp.sum((u * u).reshape(BAND // 8, 8, E), axis=0)

            sums_start(it)
        return step, ratio

    backward(0, build_laplace, g)
    d[...] = g[...]
    forward(0, lambda: None, first)
    for it in range(1, ITERS):
        backward(it, functools.partial(reg_start, it - 1), a)
        reg_end(it - 1)
        forward(it, functools.partial(dots, it - 1), functools.partial(advance, it))
    last = ITERS - 1
    norm = norms[-1]
    me = obs * 2 + c
    pls[...] = sq[...]
    plr[me] = sq[...]

    @pl.loop(1, n_plane)
    def _(i):
        pcopy(me, i).start()

    reg = rowsum(sums_end(last))

    @pl.loop(1, n_plane)
    def _(i):
        pcopy((me + i) % n_plane, i).wait_recv()

    curvature = rowsum(jnp.sum(plr[...], axis=0)) + reg
    out[...] = slip[...] + (norm / curvature) * d[...]

    @pl.loop(1, n_plane)
    def _(i):
        pcopy(me, i).wait_send()


def shards(green, data, neighbours, reg_weight):
    rows, cols = green.shape
    E = data.shape[1]
    n_obs, n_patch = lax.axis_size("obs"), lax.axis_size("patch")
    nbit = n_obs.bit_length() - 1
    nc = rows // 2 // 64
    bc = 8
    R, BR, ext = rows // 2 // nc, cols // bc, cols + 2 * BAND
    V = pltpu.VMEM
    D = pltpu.SemaphoreType.DMA
    scratch = [
        V((rows, cols), BF16), V((rows, cols), BF16),
        V((cols, rows), BF16), V((cols, rows), BF16),
        V((cols, ext), BF16), V((ext, cols), BF16),
        V((cols, 2 * E), BF16), V((rows, 2 * E), BF16), V((ext, 2 * E), BF16),
        V((cols, E), F32), V((cols, E), F32), V((cols, E), F32), V((ext, E), F32), V((cols, E), F32),
        V((8, E), F32),
        V((2, BAND, E), F32), V((2, BAND, E), F32), V((nc, R, E), F32), V((nc, R, E), F32),
        V((nc, R, E), F32), V((nc, R, E), F32), V((ITERS, nc, R, E), F32),
        V((nc, R, E), F32), V((nc, R, E), F32),
        V((ITERS, nc, R, E), F32), V((ITERS, nc, R, E), F32),
        V((ITERS - 1, 2, nc, R, E), F32),
        V((ITERS, nbit, bc, BR, E), F32), V((ITERS, nbit, bc, BR, E), F32),
        V((ITERS, 2, BAND, E), F32), V((ITERS - 1, 2, BAND, E), F32),
        V((ITERS, 8, E), F32), V((ITERS, n_patch, 8, E), F32),
        V((8, E), F32), V((2 * n_obs, 8, E), F32),
        D((2, ITERS, nc)), D((2, ITERS, nc)), D((2, ITERS, nc)), D((2, ITERS - 1, nc)),
        D((2, ITERS, nbit, bc)), D((2, ITERS, 2)), D((2, ITERS - 1, 2)),
        D((2, ITERS, n_patch)), D((2 * n_obs,)), D((2 * n_obs,)),
    ]
    return pl.pallas_call(
        functools.partial(kernel, n_obs, n_patch, nc, bc),
        out_shape=jax.ShapeDtypeStruct((cols, E), F32),
        in_specs=[pl.BlockSpec(memory_space=pltpu.VMEM)] * 4,
        out_specs=pl.BlockSpec(memory_space=pltpu.VMEM),
        scratch_shapes=scratch,
        compiler_params=pltpu.CompilerParams(
            collective_id=0, has_side_effects=True, vmem_limit_bytes=56 * 1024 * 1024),
    )(green, data, neighbours, reg_weight.reshape(1, E))


def solution(mesh):
    in_specs = (P("obs", "patch"), P("obs", None), P(None, "patch"), P())
    return jax.shard_map(shards, mesh=mesh, in_specs=in_specs, out_specs=P("patch", None), check_vma=False)
```
